32 devices in a mesh: rows: 8 (over z, y), groups: 4 (over x, core).
Axes of the slice: x: 2, y: 2, z: 4, core: 2. Of those that a mesh axis runs over, the one named last changes fastest.
Arguments:
- basis: bfloat16 [8, 131072, 128], P(None, ('rows', 'groups')), may hold values from -6 to 6
- image: bfloat16 [8, 131072, 128], P(None, ('rows', 'groups')), may hold values from -6 to 6
- selection: int32 [8, 64], replicated, may hold values from 0 to 127, all different within a row
Outputs:
- rotated: bfloat16 [8, 131072, 128], P(None, ('rows', 'groups'))
The draws below stay inside these ranges and needn't reach their ends.
Inputs may be any that keep to these rules, and one draw needn't show every extreme that they name: Each row of selection names 64 different columns.
All inputs are finite; a program needn't handle non-finite values.
Results may differ from the reference program's by a relative error of at most 0.005.
Values may be sent and summed in bfloat16 or wider, within the bound.
No kernel may reach another device: no remote copies, remote signals or barrier semaphores. Data moves between devices by JAX's collectives and lax.ppermute only.
A program may use at most 128 MiB of HBM per device.

```python
import jax
import jax.numpy as jnp
from jax import lax

RECYCLE = 64
COLS = 128
NSYS = 8
ITERS = 3
NROWS = 131072


def levels(own_key, shape, shards, smallest, largest):
    gain = 1.0
    for position, shards_of in shards:
        steps = jax.random.uniform(jax.random.fold_in(jax.random.fold_in(own_key, 6), position), (shards_of,), jnp.float32, smallest / len(shards), largest / len(shards))
        gain = gain * jnp.repeat(jnp.exp(steps), shape[position] // shards_of).reshape((-1,) + (1,) * (len(shape) - 1 - position))
    return gain


def picks_of(rng, rows, amount, top, lift):
    sequence = jax.random.permutation(jax.random.fold_in(rng, 1), amount)
    favour = sequence
    for power in range(3):
        favour = favour * favour // amount
    favour = favour * lift // amount
    chance = jax.random.randint(jax.random.fold_in(rng, 2), (rows, amount), 0, 4096) + favour
    sure = jax.random.permutation(jax.random.fold_in(rng, 3), rows)[jnp.arange(amount) % rows]
    chance = jnp.where(jnp.arange(rows)[:, None] == sure[None, :], 1 << 14, chance)
    merit = chance * amount + jnp.arange(amount)
    return lax.top_k(merit.astype(jnp.int32), top)[1].astype(jnp.int32)


def noise(key, dims, scale, limit, split=(), kind=jnp.bfloat16):
    gain = levels(key, dims, split, -0.22, 0.18) if split else 1.0
    values = jax.random.normal(key, dims, jnp.float32) * scale * gain
    return jnp.minimum(jnp.maximum(values, -limit), limit).astype(kind)


def setup_inputs(seed: int = 0) -> dict:
    streams_of = jax.random.split(jax.random.key(seed), 4)
    basis = noise(streams_of[0], (NSYS, NROWS, COLS), 1.0, 6.0, ((1, 32),))
    image = noise(streams_of[1], (NSYS, NROWS, COLS), 1.0, 6.0, ((1, 32),))
    selection = picks_of(streams_of[2], NSYS, COLS, RECYCLE, 0)
    return dict(basis=basis, image=image, selection=selection)


def small_solve(grams, chosen):
    gram_s, cross, gram_f = (grams[0], grams[1], grams[2])
    width = gram_s.shape[0]
    coeffs = (jnp.arange(width, dtype=jnp.int32)[:, None] == chosen[None, :]).astype(jnp.float32)
    factor = jnp.linalg.cholesky(gram_f)
    for step in range(ITERS):
        moved = jnp.dot(cross.T, coeffs, precision=lax.Precision.HIGHEST)
        halfway = lax.linalg.triangular_solve(factor, moved, left_side=True, lower=True)
        solved = lax.linalg.triangular_solve(factor, halfway, left_side=True, lower=True, transpose_a=True)
        metric = jnp.dot(solved.T, jnp.dot(gram_s, solved, precision=lax.Precision.HIGHEST), precision=lax.Precision.HIGHEST) / NROWS
        lower = jnp.linalg.cholesky(metric)
        coeffs = lax.linalg.triangular_solve(lower, solved, left_side=False, lower=True, transpose_a=True)
    return coeffs

def one_system(items):
    left, right, chosen = items
    gram_s = jnp.dot(left.T.astype(jnp.float32), left.astype(jnp.float32), preferred_element_type=jnp.float32)
    cross = jnp.dot(left.T.astype(jnp.float32), right.astype(jnp.float32), preferred_element_type=jnp.float32)
    gram_f = jnp.dot(right.T.astype(jnp.float32), right.astype(jnp.float32), preferred_element_type=jnp.float32)
    coeffs = small_solve(jnp.stack([gram_s, cross, gram_f]), chosen).astype(jnp.bfloat16)
    first = jnp.dot(left.astype(jnp.float32), coeffs.astype(jnp.float32), preferred_element_type=jnp.float32)
    second = jnp.dot(right.astype(jnp.float32), coeffs.astype(jnp.float32), preferred_element_type=jnp.float32)
    return jnp.concatenate([first, second], axis=1).astype(jnp.bfloat16)

def reference(basis, image, selection):
    return lax.map(one_system, (basis, image, selection))
```

```python
import functools

import jax
import jax.numpy as jnp
from jax import lax
from jax.experimental import pallas as pl
from jax.experimental.pallas import tpu as pltpu
from jax.sharding import Mesh
from jax.sharding import PartitionSpec as P

ITERS = 3
SUB = 8
HI = lax.Precision.HIGHEST


def gram_kernel(order_ref, basis_ref, image_ref, packed_ref):
    width = basis_ref.shape[2]
    pair = jnp.concatenate([basis_ref[0], image_ref[0]], axis=1)
    grams = lax.dot_general(
        pair, pair, (((0,), (0,)), ((), ())), preferred_element_type=jnp.float32
    )
    gram_s = grams[:width, :width]
    cross_t = grams[width:, :width]
    gram_f = grams[width:, width:]
    row = lax.broadcasted_iota(jnp.int32, (width, width), 0)
    col = lax.broadcasted_iota(jnp.int32, (width, width), 1)
    packed_ref[0, :width, :] = cross_t
    packed_ref[0, width : 2 * width, :] = jnp.where(row <= col, gram_s, gram_f)
    diagonal = jnp.sum(jnp.where(row == col, gram_f, 0.0), axis=0, keepdims=True)
    packed_ref[0, 2 * width :, :] = jnp.broadcast_to(diagonal, (SUB, width))


def gram(basis, image, order):
    _, rows, width = basis.shape
    count = order.shape[0]
    block = pl.BlockSpec((1, rows, width), lambda i, order: (order[i], 0, 0))
    return pl.pallas_call(
        gram_kernel,
        grid_spec=pltpu.PrefetchScalarGridSpec(
            num_scalar_prefetch=1,
            grid=(count,),
            in_specs=[block, block],
            out_specs=pl.BlockSpec((1, 2 * width + SUB, width), lambda i, order: (i, 0, 0)),
        ),
        out_shape=jax.ShapeDtypeStruct((count, 2 * width + SUB, width), jnp.float32),
        name="gram",
    )(order, basis, image)


def lanes_of(tile, column):
    return jnp.broadcast_to(tile[:, column : column + 1], tile.shape)


def row_of(tile, row):
    return jnp.broadcast_to(tile[row : row + 1, :], tile.shape)


def eliminate(square, side, forward):
    count = len(square)
    square, side = list(square), list(side)
    sub = lax.broadcasted_iota(jnp.int32, square[0].shape, 0)
    done = []
    for p in range(count):
        base = p * SUB
        pivots = [lanes_of(square[p], base + k) for k in range(SUB)]
        carried = [square[p], side[p]]
        kept = None
        for k in range(SUB):
            pivot = row_of(pivots[k], k)
            inverse = 1.0 / pivot
            if forward:
                scaled = row_of(carried[1], k) * lax.rsqrt(pivot)
                kept = scaled if k == 0 else jnp.where(sub >= k, scaled, kept)
            column, here = pivots[k], sub == k

            def reduce(tile):
                row = row_of(tile, k) * inverse
                return jnp.where(here, row, tile - column * row)

            carried = [reduce(tile) for tile in carried]
            pivots = [reduce(tile) if j > k else tile for j, tile in enumerate(pivots)]
        rows = [[row_of(tile, k) for k in range(SUB)] for tile in carried]
        others = list(range(p + 1, count))
        if forward:
            done.append(kept)
        else:
            others += list(range(p))
            square[p], side[p] = carried
        for i in others:
            weights = [lanes_of(square[i], base + k) for k in range(SUB)]

            def update(tile, row):
                terms = [weight * r for weight, r in zip(weights, row)]
                while len(terms) > 1:
                    terms = [a + b for a, b in zip(terms[::2], terms[1::2])]
                return tile - terms[0]

            square[i] = update(square[i], rows[0])
            side[i] = update(side[i], rows[1])
    return jnp.concatenate(done if forward else side, axis=0)


def tiles(matrix):
    return [matrix[i : i + SUB, :] for i in range(0, matrix.shape[0], SUB)]


def solve_kernel(total_rows, system_ref, selection_ref, first_ref, second_ref, out_ref):
    packed = first_ref[...] + second_ref[...]
    recycle, width = out_ref.shape
    dot = functools.partial(lax.dot_general, precision=HI, preferred_element_type=jnp.float32)
    rows_cols, rows_rows = (((1,), (0,)), ((), ())), (((1,), (1,)), ((), ()))
    both = packed[width : 2 * width]
    diagonal = jnp.broadcast_to(packed[2 * width : 2 * width + 1], both.shape)
    row = lax.broadcasted_iota(jnp.int32, both.shape, 0)
    col = lax.broadcasted_iota(jnp.int32, both.shape, 1)
    flipped = both.T
    gram_s = jnp.where(row <= col, both, flipped)
    gram_f = jnp.where(row > col, both, jnp.where(row < col, flipped, diagonal))
    step = eliminate(tiles(gram_f), tiles(packed[:width]), False)
    largest = jnp.max(jnp.max(jnp.abs(step), axis=1, keepdims=True), axis=0, keepdims=True)
    step_t = (step * (1.0 / largest)).T
    chosen = selection_ref[pl.ds(system_ref[0], 1), :]
    picks = lax.broadcasted_iota(jnp.int32, (width, recycle), 0) == chosen
    coeffs_t = picks.astype(jnp.float32).T
    for turn in range(ITERS):
        coeffs_t = dot(coeffs_t, step_t, rows_cols)
        if turn == 0 and ITERS > 1:
            continue
        metric = dot(dot(coeffs_t, gram_s, rows_cols), coeffs_t, rows_rows) * (1.0 / total_rows)
        metric = jnp.concatenate([metric, jnp.zeros((recycle, width - recycle), jnp.float32)], axis=1)
        coeffs_t = eliminate(tiles(metric), tiles(coeffs_t), True)
    out_ref[...] = coeffs_t.astype(out_ref.dtype)


def small_solve(first, second, selection, system, total_rows):
    vmem = pl.BlockSpec(memory_space=pltpu.VMEM)
    return pl.pallas_call(
        functools.partial(solve_kernel, total_rows),
        in_specs=[pl.BlockSpec(memory_space=pltpu.SMEM), vmem, vmem, vmem],
        out_specs=vmem,
        out_shape=jax.ShapeDtypeStruct((selection.shape[1], first.shape[1]), jnp.bfloat16),
        name="small_solve",
    )(system, selection, first, second)


def rotate_kernel(coeffs_ref, basis_ref, image_ref, out_ref):
    coeffs_t = coeffs_ref[0]
    zero = jnp.zeros_like(coeffs_t)
    weights = jnp.concatenate(
        [jnp.concatenate([coeffs_t, zero], axis=1), jnp.concatenate([zero, coeffs_t], axis=1)], axis=0
    )
    pair = jnp.concatenate([basis_ref[0], image_ref[0]], axis=1)
    out_ref[0] = lax.dot_general(
        pair, weights, (((1,), (1,)), ((), ())), preferred_element_type=jnp.float32
    ).astype(out_ref.dtype)


def rotate(basis, image, coeffs_t, parts=4):
    systems, rows, width = basis.shape
    block = pl.BlockSpec((1, rows // parts, width), lambda s, r: (s, r, 0))
    return pl.pallas_call(
        rotate_kernel,
        grid=(systems, parts),
        in_specs=[pl.BlockSpec((1,) + coeffs_t.shape[1:], lambda s, r: (s, 0, 0)), block, block],
        out_specs=block,
        out_shape=jax.ShapeDtypeStruct(basis.shape, basis.dtype),
        name="rotate",
    )(coeffs_t, basis, image)


def on_device(basis, image, selection):
    systems = basis.shape[0]
    far, near, side = (lax.axis_size(name) for name in ("far", "near", "side"))
    total_rows = basis.shape[1] * far * near * side * 2
    core = lax.axis_index("core")
    evens = 2 * jnp.arange(systems // 2, dtype=jnp.int32)
    given = gram(basis, image, evens + 1 - core)
    taken = lax.ppermute(given, "core", [(0, 1), (1, 0)])
    shares = gram(basis, image, evens + core) + taken
    pieces = lax.all_to_all(shares, ("near", "side"), 0, 0, tiled=True)
    partial = jnp.sum(pieces, axis=0)
    distance = 1
    other = jnp.zeros_like(partial)
    while distance < far:
        partial = partial + other if distance > 1 else partial
        other = lax.ppermute(partial, "far", [(i, i ^ distance) for i in range(far)])
        distance *= 2
    system = (lax.axis_index("near") * side + lax.axis_index("side")) * 2 + core
    local = small_solve(partial, other, selection, system.reshape(1), float(total_rows))
    coeffs_t = lax.all_gather(local, ("near", "side", "core"), axis=0)
    return rotate(basis, image, coeffs_t)


def solution(mesh):
    def sharded(basis, image, selection):
        rows, groups = mesh.shape["rows"], mesh.shape["groups"]
        near = basis.shape[0] // groups
        fine = Mesh(
            mesh.devices.reshape(rows // near, near, groups // 2, 2), ("far", "near", "side", "core")
        )
        split = P(None, ("far", "near", "side", "core"), None)
        run = jax.shard_map(
            on_device, mesh=fine, in_specs=(split, split, P()), out_specs=split, check_vma=False
        )
        return run(basis, image, selection)

    return sharded
```

```python
import functools

import jax
import jax.numpy as jnp
from jax import lax
from jax.experimental import pallas as pl
from jax.experimental.pallas import tpu as pltpu
from jax.sharding import Mesh
from jax.sharding import PartitionSpec as P

ITERS = 3
SUB = 8
HI = lax.Precision.HIGHEST


def systems_of(count, given):
    parity = lax.axis_index("core")
    return [2 * j + (1 - parity if given else parity) for j in range(count)]


def gram_kernel(given, ahead, basis_hbm, image_hbm, packed_ref, basis_ref, image_ref, sems):
    count, _, width = basis_ref.shape
    systems = systems_of(count, given)

    def copies(j):
        pairs = ((basis_hbm, basis_ref), (image_hbm, image_ref))
        return [
            pltpu.make_async_copy(source.at[systems[j]], kept.at[j], sems.at[j, n])
            for n, (source, kept) in enumerate(pairs)
        ]

    def product(left, right):
        return lax.dot_general(
            left, right, (((0,), (0,)), ((), ())), preferred_element_type=jnp.float32
        )

    for j in range(min(ahead, count)):
        for copy in copies(j):
            copy.start()
    row = lax.broadcasted_iota(jnp.int32, (width, width), 0)
    col = lax.broadcasted_iota(jnp.int32, (width, width), 1)
    for j in range(count):
        for copy in copies(j):
            copy.wait()
        if j + ahead < count:
            for copy in copies(j + ahead):
                copy.start()
        basis, image = basis_ref[j], image_ref[j]
        lower = product(image, jnp.concatenate([basis, image], axis=1))
        gram_s, gram_f = product(basis, basis), lower[:, width:]
        packed_ref[j, :width, :] = lower[:, :width]
        packed_ref[j, width : 2 * width, :] = jnp.where(row <= col, gram_s, gram_f)
        diagonal = jnp.sum(jnp.where(row == col, gram_f, 0.0), axis=0, keepdims=True)
        packed_ref[j, 2 * width :, :] = jnp.broadcast_to(diagonal, (SUB, width))


def gram(basis, image, given):
    systems, rows, width = basis.shape
    count = systems // 2
    hbm, vmem = pl.BlockSpec(memory_space=pltpu.HBM), pl.BlockSpec(memory_space=pltpu.VMEM)
    kept = pltpu.VMEM((count, rows, width), basis.dtype)
    return pl.pallas_call(
        functools.partial(gram_kernel, given, 3),
        in_specs=[hbm, hbm],
        out_specs=[vmem, vmem, vmem],
        out_shape=[pltpu.VMEM((count, 2 * width + SUB, width), jnp.float32), kept, kept],
        scratch_shapes=[pltpu.SemaphoreType.DMA((count, 2))],
        compiler_params=pltpu.CompilerParams(vmem_limit_bytes=16 << 20),
        name="gram",
    )(
        pltpu.with_memory_space_constraint(basis, pltpu.HBM),
        pltpu.with_memory_space_constraint(image, pltpu.HBM),
    )


def lanes_of(tile, column):
    return jnp.broadcast_to(tile[:, column : column + 1], tile.shape)


def row_of(tile, row):
    return jnp.broadcast_to(tile[row : row + 1, :], tile.shape)


def eliminate(square, side, forward):
    count = len(square)
    square, side = list(square), list(side)
    sub = lax.broadcasted_iota(jnp.int32, square[0].shape, 0)
    done = []
    for p in range(count):
        base = p * SUB
        pivots = [lanes_of(square[p], base + k) for k in range(SUB)]
        carried = [square[p], side[p]]
        kept = None
        for k in range(SUB):
            pivot = row_of(pivots[k], k)
            inverse = 1.0 / pivot
            if forward:
                scaled = row_of(carried[1], k) * lax.rsqrt(pivot)
                kept = scaled if k == 0 else jnp.where(sub >= k, scaled, kept)
            column, here = pivots[k], sub == k

            def reduce(tile):
                row = row_of(tile, k) * inverse
                return jnp.where(here, row, tile - column * row)

            carried = [reduce(tile) for tile in carried]
            pivots = [reduce(tile) if j > k else tile for j, tile in enumerate(pivots)]
        rows = [[row_of(tile, k) for k in range(SUB)] for tile in carried]
        others = list(range(p + 1, count))
        if forward:
            done.append(kept)
        else:
            others += list(range(p))
            square[p], side[p] = carried
        for i in others:
            weights = [lanes_of(square[i], base + k) for k in range(SUB)]

            def update(tile, row):
                terms = [weight * r for weight, r in zip(weights, row)]
                while len(terms) > 1:
                    terms = [a + b for a, b in zip(terms[::2], terms[1::2])]
                return tile - terms[0]

            square[i] = update(square[i], rows[0])
            side[i] = update(side[i], rows[1])
    return jnp.concatenate(done if forward else side, axis=0)


def tiles(matrix):
    return [matrix[i : i + SUB, :] for i in range(0, matrix.shape[0], SUB)]


def solve_kernel(total_rows, selection_ref, first_ref, second_ref, out_ref):
    packed = first_ref[...] + second_ref[...]
    recycle, width = out_ref.shape
    dot = functools.partial(lax.dot_general, precision=HI, preferred_element_type=jnp.float32)
    rows_cols, rows_rows = (((1,), (0,)), ((), ())), (((1,), (1,)), ((), ()))
    both = packed[width : 2 * width]
    diagonal = jnp.broadcast_to(packed[2 * width : 2 * width + 1], both.shape)
    row = lax.broadcasted_iota(jnp.int32, both.shape, 0)
    col = lax.broadcasted_iota(jnp.int32, both.shape, 1)
    flipped = both.T
    gram_s = jnp.where(row <= col, both, flipped)
    gram_f = jnp.where(row > col, both, jnp.where(row < col, flipped, diagonal))
    step = eliminate(tiles(gram_f), tiles(packed[:width]), False)
    largest = jnp.max(jnp.max(jnp.abs(step), axis=1, keepdims=True), axis=0, keepdims=True)
    step_t = (step * (1.0 / largest)).T
    plane = lax.axis_index("near") * lax.axis_size("side") + lax.axis_index("side")
    chosen = selection_ref[pl.ds(plane * 2 + lax.axis_index("core"), 1), :]
    picks = lax.broadcasted_iota(jnp.int32, (width, recycle), 0) == chosen
    coeffs_t = picks.astype(jnp.float32).T
    for turn in range(ITERS):
        coeffs_t = dot(coeffs_t, step_t, rows_cols)
        if turn == 0 and ITERS > 1:
            continue
        metric = dot(dot(coeffs_t, gram_s, rows_cols), coeffs_t, rows_rows) * (1.0 / total_rows)
        metric = jnp.concatenate([metric, jnp.zeros((recycle, width - recycle), jnp.float32)], axis=1)
        coeffs_t = eliminate(tiles(metric), tiles(coeffs_t), True)
    out_ref[...] = coeffs_t.astype(out_ref.dtype)


def add_up_kernel(pieces_ref, sum_ref):
    total = pieces_ref[0]
    for n in range(1, pieces_ref.shape[0]):
        total += pieces_ref[n]
    sum_ref[...] = total


def add_up(pieces):
    return pl.pallas_call(
        add_up_kernel,
        out_shape=jax.ShapeDtypeStruct(pieces.shape[1:], pieces.dtype),
        compiler_params=pltpu.CompilerParams(vmem_limit_bytes=8 << 20),
        name="add_up",
    )(pieces)


def small_solve(first, second, selection, total_rows):
    return pl.pallas_call(
        functools.partial(solve_kernel, total_rows),
        out_shape=jax.ShapeDtypeStruct((selection.shape[1], first.shape[1]), jnp.bfloat16),
        compiler_params=pltpu.CompilerParams(vmem_limit_bytes=16 << 20),
        name="small_solve",
    )(selection, first, second)


def rotate_kernel(coeffs_ref, *refs):
    *kept, out_hbm, staged_ref, sems = refs
    count = kept[0].shape[0]
    turns = [(kept[:2], j, s) for j, s in enumerate(systems_of(count, True))]
    turns += [(kept[2:], j, s) for j, s in enumerate(systems_of(count, False))]
    sent = []
    for turn, ((basis_ref, image_ref), j, system) in enumerate(turns):
        coeffs_t = coeffs_ref[system]
        zero = jnp.zeros_like(coeffs_t)
        weights = jnp.concatenate(
            [jnp.concatenate([coeffs_t, zero], axis=1), jnp.concatenate([zero, coeffs_t], axis=1)],
            axis=0,
        )
        pair = jnp.concatenate([basis_ref[j], image_ref[j]], axis=1)
        staged_ref[turn] = lax.dot_general(
            pair, weights, (((1,), (1,)), ((), ())), preferred_element_type=jnp.float32
        ).astype(staged_ref.dtype)
        copy = pltpu.make_async_copy(staged_ref.at[turn], out_hbm.at[system], sems.at[turn])
        copy.start()
        sent.append(copy)
    for copy in sent:
        copy.wait()


def rotate(kept, coeffs_t):
    count, rows, width = kept[0].shape
    whole = (2 * count, rows, width)
    return pl.pallas_call(
        rotate_kernel,
        in_specs=[pl.BlockSpec(memory_space=pltpu.VMEM)] * (1 + len(kept)),
        out_specs=pl.BlockSpec(memory_space=pltpu.HBM),
        out_shape=jax.ShapeDtypeStruct(whole, kept[0].dtype),
        scratch_shapes=[
            pltpu.VMEM(whole, kept[0].dtype),
            pltpu.SemaphoreType.DMA((2 * count,)),
        ],
        compiler_params=pltpu.CompilerParams(vmem_limit_bytes=24 << 20),
        name="rotate",
    )(coeffs_t, *[pltpu.with_memory_space_constraint(array, pltpu.VMEM) for array in kept])


def on_device(basis, image, selection):
    far, near, side = (lax.axis_size(name) for name in ("far", "near", "side"))
    total_rows = basis.shape[1] * far * near * side * 2
    given, *kept_given = gram(basis, image, True)
    taken = lax.ppermute(given, "core", [(0, 1), (1, 0)])
    own, *kept_own = gram(basis, image, False)
    pieces = lax.all_to_all(own + taken, ("near", "side"), 0, 0, tiled=True)
    partial = add_up(pieces)
    other = jnp.zeros_like(partial)
    distance = 1
    while distance < far:
        partial = partial + other if distance > 1 else partial
        other = lax.ppermute(partial, "far", [(i, i ^ distance) for i in range(far)])
        distance *= 2
    local = small_solve(partial, other, selection, float(total_rows))
    coeffs_t = lax.all_gather(local, ("near", "side", "core"), axis=0)
    return rotate(kept_given + kept_own, coeffs_t)


def solution(mesh):
    def sharded(basis, image, selection):
        rows, groups = mesh.shape["rows"], mesh.shape["groups"]
        near = basis.shape[0] // groups
        fine = Mesh(
            mesh.devices.reshape(rows // near, near, groups // 2, 2), ("far", "near", "side", "core")
        )
        split = P(None, ("far", "near", "side", "core"), None)
        run = jax.shard_map(
            on_device, mesh=fine, in_specs=(split, split, P()), out_specs=split, check_vma=False
        )
        return run(basis, image, selection)

    return sharded
```

```python
import functools

import jax
import jax.numpy as jnp
from jax import lax
from jax.experimental import pallas as pl
from jax.experimental.pallas import tpu as pltpu
from jax.sharding import Mesh
from jax.sharding import PartitionSpec as P

ITERS = 3
SUB = 8
HI = lax.Precision.HIGHEST


def systems_of(count, given):
    parity = lax.axis_index("core")
    return [2 * j + (1 - parity if given else parity) for j in range(count)]


def gram_kernel(given, ahead, basis_hbm, image_hbm, packed_ref, basis_ref, image_ref, sems):
    count, _, width = basis_ref.shape
    systems = systems_of(count, given)

    def copies(j):
        pairs = ((basis_hbm, basis_ref), (image_hbm, image_ref))
        return [
            pltpu.make_async_copy(source.at[systems[j]], kept.at[j], sems.at[j, n])
            for n, (source, kept) in enumerate(pairs)
        ]

    def product(left, right):
        return lax.dot_general(
            left, right, (((0,), (0,)), ((), ())), preferred_element_type=jnp.float32
        )

    for j in range(min(ahead, count)):
        for copy in copies(j):
            copy.start()
    row = lax.broadcasted_iota(jnp.int32, (width, width), 0)
    col = lax.broadcasted_iota(jnp.int32, (width, width), 1)
    for j in range(count):
        for copy in copies(j):
            copy.wait()
        if j + ahead < count:
            for copy in copies(j + ahead):
                copy.start()
        basis, image = basis_ref[j], image_ref[j]
        lower = product(image, jnp.concatenate([basis, image], axis=1))
        gram_s, gram_f = product(basis, basis), lower[:, width:]
        packed_ref[j, :width, :] = lower[:, :width]
        packed_ref[j, width : 2 * width, :] = jnp.where(row <= col, gram_s, gram_f)
        diagonal = jnp.sum(jnp.where(row == col, gram_f, 0.0), axis=0, keepdims=True)
        packed_ref[j, 2 * width :, :] = jnp.broadcast_to(diagonal, (SUB, width))


def gram(basis, image, given):
    systems, rows, width = basis.shape
    count = systems // 2
    hbm, vmem = pl.BlockSpec(memory_space=pltpu.HBM), pl.BlockSpec(memory_space=pltpu.VMEM)
    kept = pltpu.VMEM((count, rows, width), basis.dtype)
    return pl.pallas_call(
        functools.partial(gram_kernel, given, 3),
        in_specs=[hbm, hbm],
        out_specs=[vmem, vmem, vmem],
        out_shape=[pltpu.VMEM((count, 2 * width + SUB, width), jnp.float32), kept, kept],
        scratch_shapes=[pltpu.SemaphoreType.DMA((count, 2))],
        compiler_params=pltpu.CompilerParams(vmem_limit_bytes=16 << 20),
        name="gram",
    )(
        pltpu.with_memory_space_constraint(basis, pltpu.HBM),
        pltpu.with_memory_space_constraint(image, pltpu.HBM),
    )


def row_of(tile, row):
    return jnp.broadcast_to(tile[row : row + 1, :], tile.shape)


def spread(tile, column):
    lane = lax.broadcasted_iota(jnp.int32, tile.shape, 1)
    alone = [jnp.where(lane == column + k, tile, 0.0) for k in range(SUB)]
    return [jnp.broadcast_to(jnp.sum(one, axis=1, keepdims=True), tile.shape) for one in alone]


def eliminate(square_ref, side_ref, first=0, done_ref=None):
    count = square_ref.shape[0] // SUB
    sub = lax.broadcasted_iota(jnp.int32, (SUB, square_ref.shape[1]), 0)

    def rows_at(i):
        return pl.ds(pl.multiple_of(i * SUB, SUB), SUB)

    def update(tile, weights, rows):
        terms = [weight * row for weight, row in zip(weights, rows)]
        while len(terms) > 1:
            terms = [a + b for a, b in zip(terms[::2], terms[1::2])]
        return tile - terms[0]

    def turn(p, pivots):
        base = first + p * SUB
        after = jnp.minimum(p + 1, count - 1)
        pivots, kept = list(pivots), None
        carried = [square_ref[rows_at(p), :], side_ref[rows_at(p), :]]
        following = square_ref[rows_at(after), :]
        weights = spread(following, base)
        for k in range(SUB):
            pivot = row_of(pivots[k], k)
            inverse = 1.0 / pivot
            if done_ref is not None:
                scaled = row_of(carried[1], k) * lax.rsqrt(pivot)
                kept = scaled if k == 0 else jnp.where(sub >= k, scaled, kept)
            column, weight, here = pivots[k], weights[k], sub == k

            def reduce(tile):
                row = row_of(tile, k) * inverse
                return jnp.where(here, row, tile - column * row), weight * row

            square, change = reduce(carried[0])
            carried, following = [square, reduce(carried[1])[0]], following - change
            for j in range(k + 1, SUB):
                pivots[j], change = reduce(pivots[j])
                weights[j] = weights[j] - change
        rows = [[row_of(tile, k) for k in range(SUB)] for tile in carried]
        upcoming = spread(following, first + after * SUB)
        for i in range(count):
            part = slice(i * SUB, (i + 1) * SUB)
            weights = spread(square_ref[part, :], base)
            square_ref[part, :] = update(square_ref[part, :], weights, rows[0])
            side_ref[part, :] = update(side_ref[part, :], weights, rows[1])
        square_ref[rows_at(p), :], side_ref[rows_at(p), :] = carried
        if done_ref is not None:
            done_ref[rows_at(p), :] = kept
        return tuple(upcoming)

    lax.fori_loop(0, count, turn, tuple(spread(square_ref[:SUB, :], first)))


def solve_spd(matrix, side, dot, square_ref, side_ref):
    width = matrix.shape[0]
    half = width // 2
    rows_cols = (((1,), (0,)), ((), ()))
    square_ref[...], side_ref[...] = matrix[:half], side[:half]
    eliminate(square_ref, side_ref)
    upper, upper_side = square_ref[...], side_ref[...]
    both = jnp.concatenate([upper, upper_side], axis=1)
    both = jnp.concatenate([both, jnp.zeros_like(both)], axis=0)
    fill = dot(matrix[half:], both, rows_cols)
    square_ref[...] = matrix[half:] - fill[:, :width]
    side_ref[...] = side[half:] - fill[:, width:]
    eliminate(square_ref, side_ref, half)
    lower_side = side_ref[...]
    padded = jnp.concatenate([jnp.zeros_like(lower_side), lower_side], axis=0)
    return jnp.concatenate([upper_side - dot(upper, padded, rows_cols), lower_side], axis=0)


def solve_kernel(total_rows, selection_ref, first_ref, second_ref, out_ref, *scratch):
    square_ref, side_ref, done_ref = scratch
    packed = first_ref[...] + second_ref[...]
    recycle, width = out_ref.shape
    dot = functools.partial(lax.dot_general, precision=HI, preferred_element_type=jnp.float32)
    rows_cols, rows_rows = (((1,), (0,)), ((), ())), (((1,), (1,)), ((), ()))
    both = packed[width : 2 * width]
    diagonal = jnp.broadcast_to(packed[2 * width : 2 * width + 1], both.shape)
    row = lax.broadcasted_iota(jnp.int32, both.shape, 0)
    col = lax.broadcasted_iota(jnp.int32, both.shape, 1)
    flipped = both.T
    gram_s = jnp.where(row <= col, both, flipped)
    gram_f = jnp.where(row > col, both, jnp.where(row < col, flipped, diagonal))
    step = solve_spd(gram_f, packed[:width], dot, square_ref, side_ref)
    step_t = step.T
    weighted = dot(dot(step_t, gram_s, rows_cols), step, rows_cols)
    chosen = selection_ref[pl.ds(plane_index() * 2 + lax.axis_index("core"), 1), :]
    picks = lax.broadcasted_iota(jnp.int32, (width, recycle), 0) == chosen
    coeffs_t = picks.astype(jnp.float32).T
    for turn in range(ITERS):
        moved = dot(coeffs_t, step, rows_rows)
        if turn == 0 and ITERS > 1:
            largest = jnp.max(jnp.max(jnp.abs(step), axis=1, keepdims=True), axis=0, keepdims=True)
            coeffs_t = moved * (1.0 / largest)
            continue
        metric = dot(dot(coeffs_t, weighted, rows_cols), coeffs_t, rows_rows) * (1.0 / total_rows)
        metric = jnp.concatenate([metric, jnp.zeros((recycle, width - recycle), jnp.float32)], axis=1)
        square_ref[...], side_ref[...] = metric, moved
        eliminate(square_ref, side_ref, done_ref=done_ref)
        coeffs_t = done_ref[...]
    out_ref[...] = coeffs_t.astype(out_ref.dtype)


def plane_index():
    return lax.axis_index("near") * lax.axis_size("side") + lax.axis_index("side")


def combine_kernel(own_ref, taken_ref, *piece_refs):
    here = plane_index()
    for offset, piece_ref in enumerate(piece_refs):
        piece_ref[...] = own_ref[here ^ offset] + taken_ref[here ^ offset]


def combine(own, taken):
    piece = pltpu.VMEM(own.shape[1:], own.dtype)
    return pl.pallas_call(
        combine_kernel,
        out_shape=[piece] * own.shape[0],
        compiler_params=pltpu.CompilerParams(vmem_limit_bytes=8 << 20),
        name="combine",
    )(own, taken)


def add_up_kernel(*refs):
    *piece_refs, sum_ref = refs
    sum_ref[...] = functools.reduce(jnp.add, [ref[...] for ref in piece_refs])


def add_up(pieces):
    return pl.pallas_call(
        add_up_kernel,
        out_shape=pltpu.VMEM(pieces[0].shape, pieces[0].dtype),
        compiler_params=pltpu.CompilerParams(vmem_limit_bytes=8 << 20),
        name="add_up",
    )(*pieces)


def small_solve(first, second, selection, total_rows):
    return pl.pallas_call(
        functools.partial(solve_kernel, total_rows),
        out_shape=jax.ShapeDtypeStruct((selection.shape[1], first.shape[1]), jnp.bfloat16),
        scratch_shapes=[pltpu.VMEM((selection.shape[1], first.shape[1]), jnp.float32)] * 3,
        compiler_params=pltpu.CompilerParams(vmem_limit_bytes=16 << 20),
        name="small_solve",
    )(selection, first, second)


def rotate_kernel(offsets, cuts, *refs):
    coeffs, refs = refs[: len(offsets)], refs[len(offsets) :]
    kept, out_hbm, staged_ref, sems = refs[:4], *refs[-3:]
    parity = lax.axis_index("core")
    piece = staged_ref.shape[1] // cuts
    sent = []
    for n, offset in enumerate(offsets):
        place = plane_index() ^ offset
        for m in range(2):
            basis_ref, image_ref = kept[2 * m : 2 * m + 2]
            system = 2 * place + (1 - parity if m else parity)
            coeffs_t = coeffs[n][m]
            zero = jnp.zeros_like(coeffs_t)
            weights = jnp.concatenate(
                [
                    jnp.concatenate([coeffs_t, zero], axis=1),
                    jnp.concatenate([zero, coeffs_t], axis=1),
                ],
                axis=0,
            )
            for c in range(cuts):
                rows = pl.ds(c * piece, piece)
                pair = jnp.concatenate([basis_ref[place, rows], image_ref[place, rows]], axis=1)
                staged_ref[2 * n + m, rows] = lax.dot_general(
                    pair, weights, (((1,), (1,)), ((), ())), preferred_element_type=jnp.float32
                ).astype(staged_ref.dtype)
                copy = pltpu.make_async_copy(
                    staged_ref.at[2 * n + m, rows], out_hbm.at[system, rows], sems.at[2 * n + m, c]
                )
                copy.start()
                sent.append(copy)
    for copy in sent:
        copy.wait()


def rotate(kept, coeffs, offsets, done=None, cuts=2):
    count, rows, width = kept[0].shape
    kept = [pltpu.with_memory_space_constraint(array, pltpu.VMEM) for array in kept]
    vmem, hbm = pl.BlockSpec(memory_space=pltpu.VMEM), pl.BlockSpec(memory_space=pltpu.HBM)
    more = [] if done is None else [done]
    taken = len(coeffs) + len(kept)
    return pl.pallas_call(
        functools.partial(rotate_kernel, offsets, cuts),
        in_specs=[vmem] * taken + [hbm] * len(more),
        out_specs=hbm,
        out_shape=pltpu.HBM((2 * count, rows, width), kept[0].dtype),
        input_output_aliases={taken: 0} if more else {},
        scratch_shapes=[
            pltpu.VMEM((2 * len(offsets), rows, width), kept[0].dtype),
            pltpu.SemaphoreType.DMA((2 * len(offsets), cuts)),
        ],
        compiler_params=pltpu.CompilerParams(vmem_limit_bytes=24 << 20),
        name="rotate",
    )(*coeffs, *kept, *more)


def on_device(basis, image, selection):
    far, near, side = (lax.axis_size(name) for name in ("far", "near", "side"))
    total_rows = basis.shape[1] * far * near * side * 2
    plane = range(1, near * side)

    def swap(value, names, size, offset):
        return lax.ppermute(value, names, [(i, i ^ offset) for i in range(size)])

    given, *kept_given = gram(basis, image, True)
    taken = swap(given, "core", 2, 1)
    own, *kept_own = gram(basis, image, False)
    pieces = combine(own, taken)
    arrived = [swap(pieces[d], ("near", "side"), near * side, d) for d in plane]
    partial = add_up([pieces[0], *arrived])
    other = jnp.zeros_like(partial)
    distance = 1
    while distance < far:
        partial = partial + other if distance > 1 else partial
        other = swap(partial, "far", far, distance)
        distance *= 2
    mine = small_solve(partial, other, selection, float(total_rows))
    pair = jnp.stack([mine, swap(mine, "core", 2, 1)])
    pairs = [swap(pair, ("near", "side"), near * side, d) for d in plane]
    kept = kept_own + kept_given
    first = rotate(kept, [pair], [0])
    return rotate(kept, pairs, list(plane), first)


def solution(mesh):
    def sharded(basis, image, selection):
        rows, groups = mesh.shape["rows"], mesh.shape["groups"]
        near = basis.shape[0] // groups
        fine = Mesh(
            mesh.devices.reshape(rows // near, near, groups // 2, 2), ("far", "near", "side", "core")
        )
        split = P(None, ("far", "near", "side", "core"), None)
        run = jax.shard_map(
            on_device, mesh=fine, in_specs=(split, split, P()), out_specs=split, check_vma=False
        )
        return run(basis, image, selection)

    return sharded
```

```python
import functools

import jax
import jax.numpy as jnp
from jax import lax
from jax.experimental import pallas as pl
from jax.experimental.pallas import tpu as pltpu
from jax.sharding import Mesh
from jax.sharding import PartitionSpec as P

ITERS = 3
SUB = 8
HI = lax.Precision.HIGHEST


def plane_index():
    return lax.axis_index("near") * lax.axis_size("side") + lax.axis_index("side")


def system_at(offset, given):
    parity = lax.axis_index("core")
    return 2 * (plane_index() ^ offset) + (1 - parity if given else parity)


def pack_grams(packed_ref, slot, basis, image):
    width = basis.shape[1]

    def product(left, right):
        return lax.dot_general(
            left, right, (((0,), (0,)), ((), ())), preferred_element_type=jnp.float32
        )

    lower = product(image, jnp.concatenate([basis, image], axis=1))
    gram_s, gram_f = product(basis, basis), lower[:, width:]
    row = lax.broadcasted_iota(jnp.int32, (width, width), 0)
    col = lax.broadcasted_iota(jnp.int32, (width, width), 1)
    packed_ref[slot, :width, :] = lower[:, :width]
    packed_ref[slot, width : 2 * width, :] = jnp.where(row <= col, gram_s, gram_f)
    diagonal = jnp.sum(jnp.where(row == col, gram_f, 0.0), axis=0, keepdims=True)
    packed_ref[slot, 2 * width :, :] = jnp.broadcast_to(diagonal, (SUB, width))


def gram_kernel(loads, ready, group, basis_hbm, image_hbm, *refs):
    held, packed_ref, basis_ref, image_ref, sems = refs[: 2 * (ready > 0)], *refs[-4:]
    ahead = 4

    def copies(j):
        pairs = ((basis_hbm, basis_ref), (image_hbm, image_ref))
        system = system_at(*loads[j][:2])
        return [
            pltpu.make_async_copy(source.at[system], kept.at[j], sems.at[j, n])
            for n, (source, kept) in enumerate(pairs)
        ]

    def start(j):
        if j < len(loads):
            for copy in copies(j):
                copy.start()

    for j in range(ahead):
        start(j)
    skipped = early_count(held, ready)
    for j in range(ready):
        pack_grams(packed_ref, j, held[0][skipped + j], held[1][skipped + j])
    for first in range(0, len(loads), group):
        members = range(first, min(first + group, len(loads)))
        for j in members:
            for copy in copies(j):
                copy.wait()
        for j in members:
            start(j + ahead)
        for j in members:
            if loads[j][2]:
                pack_grams(packed_ref, ready + j, basis_ref[j], image_ref[j])


def early_count(held, ready):
    return held[0].shape[0] - ready if held else 0


def gram(basis, image, loads, group, ready=0, held=()):
    _, rows, width = basis.shape
    count = ready + sum(wanted for _, _, wanted in loads)
    hbm, vmem = pl.BlockSpec(memory_space=pltpu.HBM), pl.BlockSpec(memory_space=pltpu.VMEM)
    kept = pltpu.VMEM((len(loads), rows, width), basis.dtype)
    return pl.pallas_call(
        functools.partial(gram_kernel, loads, ready, group),
        in_specs=[hbm, hbm] + [vmem] * len(held),
        out_specs=[vmem, vmem, vmem],
        out_shape=[pltpu.VMEM((count, 2 * width + SUB, width), jnp.float32), kept, kept],
        scratch_shapes=[pltpu.SemaphoreType.DMA((len(loads), 2))],
        compiler_params=pltpu.CompilerParams(vmem_limit_bytes=16 << 20),
        name="gram",
    )(
        pltpu.with_memory_space_constraint(basis, pltpu.HBM),
        pltpu.with_memory_space_constraint(image, pltpu.HBM),
        *[pltpu.with_memory_space_constraint(array, pltpu.VMEM) for array in held],
    )


def row_of(tile, row):
    return jnp.broadcast_to(tile[row : row + 1, :], tile.shape)


def spread(tile, column):
    lane = lax.broadcasted_iota(jnp.int32, tile.shape, 1)
    alone = [jnp.where(lane == column + k, tile, 0.0) for k in range(SUB)]
    return [jnp.broadcast_to(jnp.sum(one, axis=1, keepdims=True), tile.shape) for one in alone]


def eliminate(square_ref, side_ref, first=0, done_ref=None):
    count = square_ref.shape[0] // SUB
    sub = lax.broadcasted_iota(jnp.int32, (SUB, square_ref.shape[1]), 0)

    def rows_at(i):
        return pl.ds(pl.multiple_of(i * SUB, SUB), SUB)

    def update(tile, weights, rows):
        terms = [weight * row for weight, row in zip(weights, rows)]
        while len(terms) > 1:
            terms = [a + b for a, b in zip(terms[::2], terms[1::2])]
        return tile - terms[0]

    def turn(p, pivots):
        base = first + p * SUB
        after = jnp.minimum(p + 1, count - 1)
        pivots, kept = list(pivots), None
        carried = [square_ref[rows_at(p), :], side_ref[rows_at(p), :]]
        following = square_ref[rows_at(after), :]
        weights = spread(following, base)
        for k in range(SUB):
            pivot = row_of(pivots[k], k)
            inverse = 1.0 / pivot
            if done_ref is not None:
                scaled = row_of(carried[1], k) * lax.rsqrt(pivot)
                kept = scaled if k == 0 else jnp.where(sub >= k, scaled, kept)
            column, weight, here = pivots[k], weights[k], sub == k

            def reduce(tile):
                row = row_of(tile, k) * inverse
                return jnp.where(here, row, tile - column * row), weight * row

            square, change = reduce(carried[0])
            carried, following = [square, reduce(carried[1])[0]], following - change
            for j in range(k + 1, SUB):
                pivots[j], change = reduce(pivots[j])
                weights[j] = weights[j] - change
        rows = [[row_of(tile, k) for k in range(SUB)] for tile in carried]
        upcoming = spread(following, first + after * SUB)
        for i in range(count):
            part = slice(i * SUB, (i + 1) * SUB)
            weights = spread(square_ref[part, :], base)
            square_ref[part, :] = update(square_ref[part, :], weights, rows[0])
            side_ref[part, :] = update(side_ref[part, :], weights, rows[1])
        square_ref[rows_at(p), :], side_ref[rows_at(p), :] = carried
        if done_ref is not None:
            done_ref[rows_at(p), :] = kept
        return tuple(upcoming)

    lax.fori_loop(0, count, turn, tuple(spread(square_ref[:SUB, :], first)))


def solve_spd(matrix, side, dot, square_ref, side_ref):
    width = matrix.shape[0]
    half = width // 2
    rows_cols = (((1,), (0,)), ((), ()))
    square_ref[...], side_ref[...] = matrix[:half], side[:half]
    eliminate(square_ref, side_ref)
    upper, upper_side = square_ref[...], side_ref[...]
    both = jnp.concatenate([upper, upper_side], axis=1)
    both = jnp.concatenate([both, jnp.zeros_like(both)], axis=0)
    fill = dot(matrix[half:], both, rows_cols)
    square_ref[...] = matrix[half:] - fill[:, :width]
    side_ref[...] = side[half:] - fill[:, width:]
    eliminate(square_ref, side_ref, half)
    lower_side = side_ref[...]
    padded = jnp.concatenate([jnp.zeros_like(lower_side), lower_side], axis=0)
    return jnp.concatenate([upper_side - dot(upper, padded, rows_cols), lower_side], axis=0)


def solve_kernel(total_rows, selection_ref, first_ref, second_ref, out_ref, *scratch):
    square_ref, side_ref, done_ref = scratch
    packed = first_ref[...] + second_ref[...]
    recycle, width = out_ref.shape
    dot = functools.partial(lax.dot_general, precision=HI, preferred_element_type=jnp.float32)
    rows_cols, rows_rows = (((1,), (0,)), ((), ())), (((1,), (1,)), ((), ()))
    both = packed[width : 2 * width]
    diagonal = jnp.broadcast_to(packed[2 * width : 2 * width + 1], both.shape)
    row = lax.broadcasted_iota(jnp.int32, both.shape, 0)
    col = lax.broadcasted_iota(jnp.int32, both.shape, 1)
    flipped = both.T
    gram_s = jnp.where(row <= col, both, flipped)
    gram_f = jnp.where(row > col, both, jnp.where(row < col, flipped, diagonal))
    step = solve_spd(gram_f, packed[:width], dot, square_ref, side_ref)
    step_t = step.T
    weighted = dot(dot(step_t, gram_s, rows_cols), step, rows_cols)
    chosen = selection_ref[pl.ds(plane_index() * 2 + lax.axis_index("core"), 1), :]
    picks = lax.broadcasted_iota(jnp.int32, (width, recycle), 0) == chosen
    coeffs_t = picks.astype(jnp.float32).T
    for turn in range(ITERS):
        moved = dot(coeffs_t, step, rows_rows)
        if turn == 0 and ITERS > 1:
            largest = jnp.max(jnp.max(jnp.abs(step), axis=1, keepdims=True), axis=0, keepdims=True)
            coeffs_t = moved * (1.0 / largest)
            continue
        metric = dot(dot(coeffs_t, weighted, rows_cols), coeffs_t, rows_rows) * (1.0 / total_rows)
        metric = jnp.concatenate([metric, jnp.zeros((recycle, width - recycle), jnp.float32)], axis=1)
        square_ref[...], side_ref[...] = metric, moved
        eliminate(square_ref, side_ref, done_ref=done_ref)
        coeffs_t = done_ref[...]
    out_ref[...] = coeffs_t.astype(out_ref.dtype)


def combine_kernel(own_ref, taken_ref, *piece_refs):
    for offset, piece_ref in enumerate(piece_refs):
        piece_ref[...] = own_ref[offset] + taken_ref[offset]


def combine(own, taken):
    piece = pltpu.VMEM(own.shape[1:], own.dtype)
    return pl.pallas_call(
        combine_kernel,
        out_shape=[piece] * own.shape[0],
        compiler_params=pltpu.CompilerParams(vmem_limit_bytes=8 << 20),
        name="combine",
    )(own, taken)


def add_up_kernel(*refs):
    *piece_refs, sum_ref = refs
    sum_ref[...] = functools.reduce(jnp.add, [ref[...] for ref in piece_refs])


def add_up(pieces):
    return pl.pallas_call(
        add_up_kernel,
        out_shape=pltpu.VMEM(pieces[0].shape, pieces[0].dtype),
        compiler_params=pltpu.CompilerParams(vmem_limit_bytes=8 << 20),
        name="add_up",
    )(*pieces)


def small_solve(first, second, selection, total_rows):
    return pl.pallas_call(
        functools.partial(solve_kernel, total_rows),
        out_shape=jax.ShapeDtypeStruct((selection.shape[1], first.shape[1]), jnp.bfloat16),
        scratch_shapes=[pltpu.VMEM((selection.shape[1], first.shape[1]), jnp.float32)] * 3,
        compiler_params=pltpu.CompilerParams(vmem_limit_bytes=16 << 20),
        name="small_solve",
    )(selection, first, second)


def rotate_kernel(offsets, cuts, *refs):
    coeffs, refs = refs[: len(offsets)], refs[len(offsets) :]
    early, late, out_hbm, staged_ref, sems = refs[:2], refs[2:4], *refs[-3:]
    plane = (early[0].shape[0] + late[0].shape[0]) // 2
    ready = plane - late[0].shape[0]
    piece = staged_ref.shape[1] // cuts
    sent = []
    for n, offset in enumerate(offsets):
        for m, given in enumerate((False, True)):
            if given:
                kept, slot = early, offset
            else:
                kept, slot = (early, plane + offset) if offset < ready else (late, offset - ready)
            system = system_at(offset, given)
            coeffs_t = coeffs[n][m]
            zero = jnp.zeros_like(coeffs_t)
            weights = jnp.concatenate(
                [
                    jnp.concatenate([coeffs_t, zero], axis=1),
                    jnp.concatenate([zero, coeffs_t], axis=1),
                ],
                axis=0,
            )
            for c in range(cuts):
                rows = pl.ds(c * piece, piece)
                pair = jnp.concatenate([kept[0][slot, rows], kept[1][slot, rows]], axis=1)
                staged_ref[2 * n + m, rows] = lax.dot_general(
                    pair, weights, (((1,), (1,)), ((), ())), preferred_element_type=jnp.float32
                ).astype(staged_ref.dtype)
                copy = pltpu.make_async_copy(
                    staged_ref.at[2 * n + m, rows], out_hbm.at[system, rows], sems.at[2 * n + m, c]
                )
                copy.start()
                sent.append(copy)
    for copy in sent:
        copy.wait()


def rotate(kept, coeffs, offsets, systems, done=None, cuts=2):
    _, rows, width = kept[0].shape
    kept = [pltpu.with_memory_space_constraint(array, pltpu.VMEM) for array in kept]
    vmem, hbm = pl.BlockSpec(memory_space=pltpu.VMEM), pl.BlockSpec(memory_space=pltpu.HBM)
    more = [] if done is None else [done]
    taken = len(coeffs) + len(kept)
    return pl.pallas_call(
        functools.partial(rotate_kernel, offsets, cuts),
        in_specs=[vmem] * taken + [hbm] * len(more),
        out_specs=hbm,
        out_shape=pltpu.HBM((systems, rows, width), kept[0].dtype),
        input_output_aliases={taken: 0} if more else {},
        scratch_shapes=[
            pltpu.VMEM((2 * len(offsets), rows, width), kept[0].dtype),
            pltpu.SemaphoreType.DMA((2 * len(offsets), cuts)),
        ],
        compiler_params=pltpu.CompilerParams(vmem_limit_bytes=24 << 20),
        name="rotate",
    )(*coeffs, *kept, *more)


def on_device(basis, image, selection):
    far, near, side = (lax.axis_size(name) for name in ("far", "near", "side"))
    total_rows = basis.shape[1] * far * near * side * 2
    plane = range(1, near * side)

    def swap(value, names, size, offset):
        return lax.ppermute(value, names, [(i, i ^ offset) for i in range(size)])

    ready = 1
    early_loads = [(d, True, True) for d in range(near * side)]
    early_loads += [(d, False, False) for d in range(ready)]
    given, *early = gram(basis, image, early_loads, 1)
    taken = swap(given, "core", 2, 1)
    late_loads = [(d, False, True) for d in range(ready, near * side)]
    own, *late = gram(basis, image, late_loads, 1, ready, early)
    pieces = combine(own, taken)
    arrived = [swap(pieces[d], ("near", "side"), near * side, d) for d in plane]
    partial = add_up([pieces[0], *arrived])
    other = jnp.zeros_like(partial)
    distance = 1
    while distance < far:
        partial = partial + other if distance > 1 else partial
        other = swap(partial, "far", far, distance)
        distance *= 2
    mine = small_solve(partial, other, selection, float(total_rows))
    pair = jnp.stack([mine, swap(mine, "core", 2, 1)])
    pairs = [swap(pair, ("near", "side"), near * side, d) for d in plane]
    first = rotate(early + late, [pair], [0], basis.shape[0])
    return rotate(early + late, pairs, list(plane), basis.shape[0], first)


def solution(mesh):
    def sharded(basis, image, selection):
        rows, groups = mesh.shape["rows"], mesh.shape["groups"]
        near = basis.shape[0] // groups
        fine = Mesh(
            mesh.devices.reshape(rows // near, near, groups // 2, 2), ("far", "near", "side", "core")
        )
        split = P(None, ("far", "near", "side", "core"), None)
        run = jax.shard_map(
            on_device, mesh=fine, in_specs=(split, split, P()), out_specs=split, check_vma=False
        )
        return run(basis, image, selection)

    return sharded
```
